128 devices in a mesh: owner: 4 (over x), rows: 32 (over z, y, core).
Axes of the slice: x: 4, y: 4, z: 4, core: 2. Of those that a mesh axis runs over, the one named last changes fastest.
Arguments:
- w_gate: float32 [64, 2048, 1024], P('owner', 'rows'), may hold values from -0.25 to 0.25
- avg_gate: bfloat16 [64, 2048, 1024], P('owner', 'rows'), may hold values from -0.0625 to 0.0625
- w_up: float32 [64, 2048, 1024], P('owner', 'rows'), may hold values from -0.25 to 0.25
- avg_up: bfloat16 [64, 2048, 1024], P('owner', 'rows'), may hold values from -0.0625 to 0.0625
- w_down: float32 [64, 1024, 2048], P('owner', None, 'rows'), may hold values from -0.375 to 0.375
- avg_down: bfloat16 [64, 1024, 2048], P('owner', None, 'rows'), may hold values from -0.09375 to 0.09375
- router_weight: float32 [2048, 64], P('rows', 'owner'), may hold values from -0.125 to 0.125
- router_gain: float32 [2048], P('rows'), may hold values from 0.25 to 1.75
Outputs:
- serve_gate: bfloat16 [64, 2048, 1024], P('owner', None, 'rows')
- serve_up: bfloat16 [64, 2048, 1024], P('owner', None, 'rows')
- serve_down: bfloat16 [64, 1024, 2048], P('owner', 'rows')
- scale_gate: float32 [64, 1024], P('owner', 'rows')
- scale_up: float32 [64, 1024], P('owner', 'rows')
- scale_down: float32 [64, 1024], P('owner', 'rows')
- serve_router: bfloat16 [2048, 64], replicated
The draws below stay inside these ranges and needn't reach their ends.
All inputs are finite; a program needn't handle non-finite values.
Results may differ from the reference program's by a relative error of at most 0.0015.
Values may be sent and summed in bfloat16 or wider, within the bound.
No kernel may reach another device: no remote copies, remote signals or barrier semaphores. Data moves between devices by JAX's collectives and lax.ppermute only.
A program may use at most 128 MiB of HBM per device.

```python
import jax
import jax.numpy as jnp
from jax import lax

EXPERTS = 64
D_MODEL = 2048
D_EXPERT = 1024


def raised(drawn, stream_key, source, target, shards_of, factor):
    owner, partner = [(jnp.arange(drawn.shape[position]) // (drawn.shape[position] // shards_of)).reshape([-1 if axis == position else 1 for axis in range(drawn.ndim)]) for position in (source, target)]
    chosen = jax.random.permutation(stream_key, shards_of)[partner]
    strong = (owner == chosen) | (owner == (partner + shards_of // 2) % shards_of)
    return jnp.where(strong, factor * drawn, drawn)


def shard_levels(key, dims, shards, smallest, top_value):
    factor_of = 1.0
    for position, blocks in shards:
        draws = jax.random.uniform(jax.random.fold_in(jax.random.fold_in(key, 6), position), (blocks,), jnp.float32, smallest / len(shards), top_value / len(shards))
        factor_of = factor_of * jnp.repeat(jnp.exp(draws), dims[position] // blocks).reshape((-1,) + (1,) * (len(dims) - 1 - position))
    return factor_of


def centred(own_key, dims, spread, limit, pieces=(), held_as=jnp.bfloat16):
    factor_of = shard_levels(own_key, dims, pieces, -0.22, 0.18) if pieces else 1.0
    entries = jax.random.normal(own_key, dims, jnp.float32) * spread * factor_of
    return jnp.minimum(jnp.maximum(entries, -limit), limit).astype(held_as)


def noise_with(stream_key, shape, deviation, limit, cuts, heavy, dtype=jnp.bfloat16):
    result = deviation * jax.random.normal(stream_key, shape, jnp.float32)
    if cuts:
        result = result * shard_levels(stream_key, shape, cuts, -0.22, 0.18)
    return jnp.clip(raised(result, jax.random.fold_in(stream_key, 3), *heavy), -limit, limit).astype(dtype)


def setup_inputs(seed: int = 0) -> dict:
    streams_of = jax.random.split(jax.random.key(seed), 9)
    w_gate = noise_with(streams_of[0], (EXPERTS, D_MODEL, D_EXPERT), D_MODEL ** -0.5, 0.25, ((0, 4), (1, 32)), (1, 2, 32, 2.75), jnp.float32)
    avg_gate = centred(streams_of[1], (EXPERTS, D_MODEL, D_EXPERT), (D_MODEL * 4) ** -0.5, 0.0625, ((0, 4), (1, 32)))
    w_up = noise_with(streams_of[2], (EXPERTS, D_MODEL, D_EXPERT), D_MODEL ** -0.5, 0.25, ((0, 4), (1, 32)), (1, 2, 32, 2.75), jnp.float32)
    avg_up = centred(streams_of[3], (EXPERTS, D_MODEL, D_EXPERT), (D_MODEL * 4) ** -0.5, 0.0625, ((0, 4), (1, 32)))
    w_down = noise_with(streams_of[4], (EXPERTS, D_EXPERT, D_MODEL), D_EXPERT ** -0.5, 0.375, ((0, 4), (2, 32)), (2, 1, 32, 2.75), jnp.float32)
    avg_down = centred(streams_of[5], (EXPERTS, D_EXPERT, D_MODEL), (D_EXPERT * 4) ** -0.5, 0.09375, ((0, 4), (2, 32)))
    router_weight = centred(streams_of[6], (D_MODEL, EXPERTS), D_MODEL ** -0.5, 0.125, ((0, 32), (1, 4)), jnp.float32)
    router_gain = jnp.clip(1.0 + 0.15 * jax.random.normal(streams_of[7], (D_MODEL,), jnp.float32), 0.25, 1.75)
    return {"w_gate": w_gate, "avg_gate": avg_gate, "w_up": w_up, "avg_up": avg_up, "w_down": w_down, "avg_down": avg_down, "router_weight": router_weight, "router_gain": router_gain}


def reference(w_gate, avg_gate, w_up, avg_up, w_down, avg_down, router_weight, router_gain):
    fresh_gate = w_gate + avg_gate.astype(jnp.float32)
    fresh_up = w_up + avg_up.astype(jnp.float32)
    fresh_down = w_down + avg_down.astype(jnp.float32)
    scale_gate = jnp.sqrt(lax.optimization_barrier(jnp.sum(fresh_gate * fresh_gate, axis=1)))
    serve_gate = (fresh_gate / jnp.expand_dims(scale_gate, 1)).astype(jnp.bfloat16)
    scale_up = jnp.sqrt(lax.optimization_barrier(jnp.sum(fresh_up * fresh_up, axis=1)))
    serve_up = (fresh_up / jnp.expand_dims(scale_up, 1)).astype(jnp.bfloat16)
    scale_down = jnp.sqrt(lax.optimization_barrier(jnp.sum(fresh_down * fresh_down, axis=2)))
    serve_down = (fresh_down / jnp.expand_dims(scale_down, 2)).astype(jnp.bfloat16)
    serve_router = (router_weight * router_gain[:, None]).astype(jnp.bfloat16)
    return (serve_gate, serve_up, serve_down, scale_gate, scale_up, scale_down, serve_router)
```

```python
import jax
import jax.numpy as jnp
from jax import lax
from jax.experimental import pallas as pl
from jax.experimental.pallas import tpu as pltpu
from jax.sharding import PartitionSpec as P

GROUPS = 4
PACK = 4
DESTS = 32
LANES = 128


def block_transpose(x):
    lane = lax.broadcasted_iota(jnp.int32, x[0].shape, 1)
    low = lane < 64
    y = [None] * 4
    for e in (0, 1):
        a, b = x[e], x[e + 2]
        y[e] = jnp.where(low, a, pltpu.roll(b, 64, 1))
        y[e + 2] = jnp.where(low, pltpu.roll(a, 64, 1), b)
    even = (lane // 32) % 2 == 0
    out = [None] * 4
    for q in (0, 2):
        a, b = y[q], y[q + 1]
        out[q] = jnp.where(even, a, pltpu.roll(b, 32, 1))
        out[q + 1] = jnp.where(even, pltpu.roll(a, 96, 1), b)
    return out


def fresh_kernel(wg, ag, wu, au, wd, ad, packed, sums):
    g = pl.program_id(0)
    for kind, (w, a) in enumerate(((wg, ag), (wu, au), (wd, ad))):
        for t in range(1024 // LANES):
            at = slice(t * LANES, (t + 1) * LANES)
            x = [w[e, :, at] + a[e, :, at].astype(jnp.float32) for e in range(PACK)]
            for q, o in enumerate(block_transpose(x)):
                d = 4 * t + q
                packed[d, kind, 0] = o
                sums[d, pl.ds(kind * GROUPS + g, 1), :] = jnp.sum(o * o, axis=0, keepdims=True)


def fresh_and_sums(w_gate, avg_gate, w_up, avg_up, w_down, avg_down):
    spec = pl.BlockSpec((PACK, 64, 1024), lambda g: (g, 0, 0))
    return pl.pallas_call(
        fresh_kernel,
        grid=(GROUPS,),
        in_specs=[spec] * 6,
        out_specs=[
            pl.BlockSpec((DESTS, 3, 1, 64, LANES), lambda g: (0, 0, g, 0, 0)),
            pl.BlockSpec((DESTS, 16, LANES), lambda g: (0, 0, 0)),
        ],
        out_shape=[
            jax.ShapeDtypeStruct((DESTS, 3, GROUPS, 64, LANES), jnp.float32),
            jax.ShapeDtypeStruct((DESTS, 16, LANES), jnp.float32),
        ],
        compiler_params=pltpu.CompilerParams(vmem_limit_bytes=48 * 2**20),
        name="fresh_and_sums",
    )(w_gate, avg_gate, w_up, avg_up, w_down, avg_down)


def scale_kernel(packed, inverse, out):
    for d in range(packed.shape[0]):
        for k in range(3 * GROUPS):
            x = packed[d, k // GROUPS, k % GROUPS] * inverse[d, k : k + 1, :]
            out[d, k * 64 : (k + 1) * 64, :] = x.astype(jnp.bfloat16)


def scaled(packed, inverse):
    step = 4
    return pl.pallas_call(
        scale_kernel,
        grid=(DESTS // step,),
        in_specs=[
            pl.BlockSpec((step, 3, GROUPS, 64, LANES), lambda i: (i, 0, 0, 0, 0)),
            pl.BlockSpec((step, 16, LANES), lambda i: (i, 0, 0)),
        ],
        out_specs=pl.BlockSpec((step, 3 * GROUPS * 64, LANES), lambda i: (i, 0, 0)),
        out_shape=jax.ShapeDtypeStruct((DESTS, 3 * GROUPS * 64, LANES), jnp.bfloat16),
        name="scaled",
    )(packed, inverse)


def unpack_kernel(g_in, u_in, d_in, g_out, u_out, d_out):
    for src, dst in ((g_in, g_out), (u_in, u_out), (d_in, d_out)):
        for s in range(0, DESTS, 2):
            x = jnp.concatenate([src[s], src[s + 1]], axis=0).astype(jnp.float32)
            y = x.T.astype(jnp.bfloat16)
            dst[:, :, s * 64 : (s + 2) * 64] = y.reshape(PACK, 32, LANES)


def unpacked(received):
    def view(kind):
        return pl.BlockSpec((DESTS, 64, LANES), lambda g: (0, kind * GROUPS + g, 0))

    return pl.pallas_call(
        unpack_kernel,
        grid=(GROUPS,),
        in_specs=[view(0), view(1), view(2)],
        out_specs=[pl.BlockSpec((PACK, 32, 2048), lambda g: (g, 0, 0))] * 3,
        out_shape=[jax.ShapeDtypeStruct((16, 32, 2048), jnp.bfloat16)] * 3,
        name="unpacked",
    )(received, received, received)


def exchanged(x):
    return lax.all_to_all(x, "rows", split_axis=0, concat_axis=0, tiled=True)


def shards(w_gate, avg_gate, w_up, avg_up, w_down, avg_down, router_weight, router_gain):
    packed, sums = fresh_and_sums(
        w_gate, avg_gate, w_up, avg_up, jnp.swapaxes(w_down, 1, 2), jnp.swapaxes(avg_down, 1, 2)
    )
    scale = jnp.sqrt(jnp.sum(exchanged(sums)[:, : 3 * GROUPS], axis=0))
    inverse = jnp.pad(1.0 / scale, ((0, 4), (0, 0)))
    inverse = exchanged(jnp.broadcast_to(inverse, (DESTS, 16, LANES)))
    payload = scaled(packed, inverse)
    received = exchanged(payload)
    serve_gate, serve_up, serve_down = unpacked(received)
    scale_gate, scale_up, scale_down = (
        scale[kind * GROUPS : (kind + 1) * GROUPS].reshape(16, 32) for kind in range(3)
    )
    part = (router_weight * router_gain[:, None]).astype(jnp.bfloat16).T
    rows = exchanged(jnp.broadcast_to(part.reshape(1, 8, LANES), (DESTS, 8, LANES)))
    rows = rows.reshape(DESTS, 16, 64).swapaxes(0, 1).reshape(16, 2048)
    owners = lax.axis_size("owner")
    me = lax.axis_index("owner")
    whole = jnp.zeros((owners, 16, 2048), jnp.bfloat16)
    whole = lax.dynamic_update_index_in_dim(whole, rows, me, 0)
    for hop in range(1, owners):
        came = lax.ppermute(rows, "owner", [(s, (s + hop) % owners) for s in range(owners)])
        whole = lax.dynamic_update_index_in_dim(whole, came, (me - hop) % owners, 0)
    serve_router = whole.reshape(64, 2048).T
    return (
        serve_gate.swapaxes(1, 2),
        serve_up.swapaxes(1, 2),
        serve_down,
        scale_gate,
        scale_up,
        scale_down,
        serve_router,
    )


def solution(mesh):
    return jax.shard_map(
        shards,
        mesh=mesh,
        in_specs=(
            P("owner", "rows", None),
            P("owner", "rows", None),
            P("owner", "rows", None),
            P("owner", "rows", None),
            P("owner", None, "rows"),
            P("owner", None, "rows"),
            P("rows", "owner"),
            P("rows"),
        ),
        out_specs=(
            P("owner", None, "rows"),
            P("owner", None, "rows"),
            P("owner", "rows", None),
            P("owner", "rows"),
            P("owner", "rows"),
            P("owner", "rows"),
            P(),
        ),
        check_vma=False,
    )
```

```python
import functools

import jax
import jax.numpy as jnp
from jax import lax
from jax.experimental import pallas as pl
from jax.experimental.pallas import tpu as pltpu
from jax.sharding import PartitionSpec as P

PACK = 4
DESTS = 32
LANES = 128
ROWS = 3 * 64 + 8
CHUNKS = ((0, 2), (2, 2))
SPAN = 2.0**-7.75


def block_transpose(x):
    lane = lax.broadcasted_iota(jnp.int32, x[0].shape, 1)
    low = lane < 64
    y = [None] * 4
    for e in (0, 1):
        a, b = x[e], x[e + 2]
        y[e] = jnp.where(low, a, pltpu.roll(b, 64, 1))
        y[e + 2] = jnp.where(low, pltpu.roll(a, 64, 1), b)
    even = (lane // 32) % 2 == 0
    out = [None] * 4
    for q in (0, 2):
        a, b = y[q], y[q + 1]
        out[q] = jnp.where(even, a, pltpu.roll(b, 32, 1))
        out[q + 1] = jnp.where(even, pltpu.roll(a, 96, 1), b)
    return out


def pack_kernel(wg, ag, wu, au, wd, ad, router, out):
    row = lax.broadcasted_iota(jnp.int32, (8, LANES), 0)
    for t in range(1024 // LANES):
        at = slice(t * LANES, (t + 1) * LANES)
        extra = [router[0]] * 4
        for kind, (w, a) in enumerate(((wg, ag), (wu, au), (wd, ad))):
            x = [w[e, :, at] + a[e, :, at].astype(jnp.float32) for e in range(PACK)]
            for q, o in enumerate(block_transpose(x)):
                top = jnp.max(jnp.abs(o), axis=0, keepdims=True)
                factor = (jnp.maximum(top, 1e-30) * SPAN).astype(jnp.bfloat16).astype(jnp.float32)
                o = o * (1.0 / factor)
                p = o * o
                p = p * p
                p = p * p
                p = p * p
                p = jnp.where(o < 0, -p, p)
                out[4 * t + q, kind * 64 : (kind + 1) * 64, :] = p.astype(jnp.bfloat16)
                extra[q] = jnp.where(row == kind, factor, extra[q])
        for q in range(4):
            out[4 * t + q, 192:200, :] = extra[q].astype(jnp.bfloat16)


def packed(first, groups, args, router):
    spec = pl.BlockSpec((PACK, 64, 1024), lambda g: (first + g, 0, 0))
    args = [pltpu.with_memory_space_constraint(a, pltpu.HBM) for a in args]
    return pl.pallas_call(
        pack_kernel,
        grid=(groups,),
        in_specs=[spec] * 6 + [pl.BlockSpec((1, 8, LANES), lambda g: (g, 0, 0))],
        out_specs=pl.BlockSpec((DESTS, ROWS, LANES), lambda g: (0, g, 0)),
        out_shape=pltpu.HBM((DESTS, groups * ROWS, LANES), jnp.bfloat16),
        compiler_params=pltpu.CompilerParams(vmem_limit_bytes=40 * 2**20),
        name="packed",
    )(*args, router)


def unpack_kernel(first, received, *refs):
    before, refs = refs[:3], refs[6:]
    serves, scales, x = refs[:3], refs[3:6], refs[6]
    g = first + pl.program_id(0)

    @pl.when(pl.program_id(0) == 0)
    def _():
        for old, new in zip(before, scales):
            new[...] = old[...]

    for kind in range(3):
        total = jnp.zeros((8, LANES), jnp.float32)
        for s in range(DESTS):
            y = received[s, kind * 64 : (kind + 1) * 64, :].astype(jnp.float32)
            factor = received[s, 192:200, :].astype(jnp.float32)[kind : kind + 1]
            root = jnp.exp2(jnp.log2(jnp.abs(y)) * 0.0625) * factor
            v = jnp.where(y < 0, -root, root)
            x[s * 64 : (s + 1) * 64, :] = v
            total = total + jnp.sum((v * v).reshape(8, 8, LANES), axis=0)
        scale = jnp.sqrt(jnp.sum(total, axis=0, keepdims=True))
        for e in range(PACK):
            scales[kind][pl.ds(g * PACK + e, 1), :] = scale[:, 32 * e : 32 * (e + 1)]
        inverse = 1.0 / scale
        for s in range(0, 2048, LANES):
            z = (x[s : s + LANES, :] * inverse).T.astype(jnp.bfloat16)
            serves[kind][:, :, s : s + LANES] = z.reshape(PACK, 32, LANES)


def unpacked(first, groups, received, serves, scales):
    whole = pl.BlockSpec((16, 32), lambda g: (0, 0))
    return pl.pallas_call(
        functools.partial(unpack_kernel, first),
        grid=(groups,),
        in_specs=[pl.BlockSpec((DESTS, ROWS, LANES), lambda g: (0, g, 0))]
        + [whole] * 3
        + [pl.BlockSpec(memory_space=pl.ANY)] * 3,
        out_specs=[pl.BlockSpec((PACK, 32, 2048), lambda g: (first + g, 0, 0))] * 3 + [whole] * 3,
        out_shape=[pltpu.HBM((16, 32, 2048), jnp.bfloat16)] * 3
        + [jax.ShapeDtypeStruct((16, 32), jnp.float32)] * 3,
        input_output_aliases={4: 0, 5: 1, 6: 2},
        scratch_shapes=[pltpu.VMEM((2048, LANES), jnp.float32)],
        compiler_params=pltpu.CompilerParams(vmem_limit_bytes=40 * 2**20),
        name="unpacked",
    )(received, *scales, *serves)


def exchanged(x):
    return lax.all_to_all(x, "rows", split_axis=0, concat_axis=0, tiled=True)


def over_owners(rows):
    owners, me = lax.axis_size("owner"), lax.axis_index("owner")
    whole = jnp.zeros((owners, *rows.shape), rows.dtype)
    whole = lax.dynamic_update_index_in_dim(whole, rows, me, 0)
    for hop in range(1, owners):
        came = lax.ppermute(rows, "owner", [(s, (s + hop) % owners) for s in range(owners)])
        whole = lax.dynamic_update_index_in_dim(whole, came, (me - hop) % owners, 0)
    return whole


def shards(w_gate, avg_gate, w_up, avg_up, w_down, avg_down, router_weight, router_gain):
    args = (w_gate, avg_gate, w_up, avg_up, jnp.swapaxes(w_down, 1, 2), jnp.swapaxes(avg_down, 1, 2))
    part = (router_weight * router_gain[:, None]).astype(jnp.bfloat16).astype(jnp.float32).T
    first_groups = CHUNKS[0][1]
    part = part.reshape(first_groups, 8 // first_groups, LANES)
    part = jnp.pad(part, ((0, 0), (8 - part.shape[1], 0), (0, 0)))
    blank = jnp.zeros_like(part)
    serves = [jnp.zeros((16, 32, 2048), jnp.bfloat16)] * 3
    scales = [jnp.zeros((16, 32), jnp.float32)] * 3
    for n, (first, groups) in enumerate(CHUNKS):
        received = exchanged(packed(first, groups, args, blank if n else part))
        outs = unpacked(first, groups, received, serves, scales)
        serves, scales = outs[:3], outs[3:]
        if n == 0:
            rows = received.reshape(DESTS, groups, ROWS, LANES)[:, :, ROWS - 8 // groups :, :]
            rows = rows.reshape(DESTS, 16, 64).swapaxes(0, 1).reshape(16, 2048)
            serve_router = over_owners(rows).reshape(64, 2048).T
    serve_gate, serve_up, serve_down = serves
    return (
        serve_gate.swapaxes(1, 2),
        serve_up.swapaxes(1, 2),
        serve_down,
        *scales,
        serve_router,
    )


def solution(mesh):
    return jax.shard_map(
        shards,
        mesh=mesh,
        in_specs=(
            P("owner", "rows", None),
            P("owner", "rows", None),
            P("owner", "rows", None),
            P("owner", "rows", None),
            P("owner", None, "rows"),
            P("owner", None, "rows"),
            P("rows", "owner"),
            P("rows"),
        ),
        out_specs=(
            P("owner", None, "rows"),
            P("owner", None, "rows"),
            P("owner", "rows", None),
            P("owner", "rows"),
            P("owner", "rows"),
            P("owner", "rows"),
            P(),
        ),
        check_vma=False,
    )
```

```python
import functools

import jax
import jax.numpy as jnp
from jax import lax
from jax.experimental import pallas as pl
from jax.experimental.pallas import tpu as pltpu
from jax.sharding import PartitionSpec as P


PACK = 4
DESTS = 32
LANES = 128
ROWS = 3 * 64 + 8
SPAN = 2.0**-7.75
BF16, F32 = jnp.bfloat16, jnp.float32


def coded(w, a, expert, at):
    x = w[expert, :, at] + a[expert, :, at].astype(F32)
    if expert:
        x = pltpu.roll(x, 32 * expert, 1)
    top = jnp.max(jnp.abs(x), axis=0, keepdims=True)
    factor = (jnp.maximum(top, 1e-30) * SPAN).astype(BF16).astype(F32)
    x = x * (1.0 / factor)
    p = x * x
    p = p * p
    p = p * p
    p = p * p
    return jnp.where(x < 0, -p, p).astype(BF16), jnp.broadcast_to(factor, (8, LANES))


def picked(q, block, rolled):
    a, b, c, d = rolled
    d = jnp.where(block == (q + 2) % 4, c, d)
    return jnp.where(block == q, a, jnp.where(block == (q + 1) % 4, b, d))


def packed_tile(families, at, put):
    wide = lax.broadcasted_iota(jnp.int32, (64, LANES), 1) // 32
    block = lax.broadcasted_iota(jnp.int32, (8, LANES), 1) // 32
    row = lax.broadcasted_iota(jnp.int32, (8, LANES), 0)
    extra = [jnp.zeros((8, LANES), F32)] * 4
    for kind, (w, a) in enumerate(families):
        codes, factors = zip(*(coded(w, a, e, at) for e in range(PACK)))
        for q in range(4):
            put(q, kind * 64, picked(q, wide, codes))
            extra[q] = jnp.where(row == kind, picked(q, block, factors), extra[q])
    for q in range(4):
        put(q, 192, extra[q].astype(BF16))


def pack_kernel(group, mode, me, *refs):
    arrays, refs = refs[:6], refs[6:]
    if group == 0:
        router, refs = refs[0], refs[1:]
    outs, refs = (refs[:1], refs[1:]) if mode == "direct" else (refs[:4], refs[4:])
    bufs, ready, in_sems, out_sems = refs[:6], refs[6], refs[7], refs[8]
    order = (0, 1, 2, 3) if mode == "direct" else (1, 2, 3, 0)

    def fetch(hops, n):
        z = hops if mode == "direct" else (me[0] + hops) & 3
        lanes = pl.ds(pl.multiple_of(z * 256, 256), 256)
        src = arrays[n].at[pl.ds(group * PACK, PACK), :, lanes]
        return pltpu.make_async_copy(src, bufs[n].at[hops], in_sems.at[hops, n])

    def give(hops):
        if mode == "direct":
            part = pl.ds(8 * hops, 8)
            return [pltpu.make_async_copy(ready.at[hops], outs[0].at[part], out_sems.at[hops, 0])]
        if mode == "z":
            return [pltpu.make_async_copy(ready.at[hops], outs[hops], out_sems.at[hops, 0])]
        return [
            pltpu.make_async_copy(ready.at[j, :, hops], outs[j].at[:, hops], out_sems.at[hops, j])
            for j in range(4)
        ]

    for hops in order:
        for n in range(6):
            fetch(hops, n).start()
    for hops in order:
        for n in range(6):
            fetch(hops, n).wait()
        families = [(bufs[2 * kind].at[hops], bufs[2 * kind + 1].at[hops]) for kind in range(3)]
        for t in range(2):

            def put(q, first, rows, t=t, hops=hops):
                at = pl.ds(first, rows.shape[0])
                core = (q % 2 + me[2]) & 1
                along = (2 * t + q // 2 - me[1]) & 3
                if mode == "direct":
                    ready[hops, 4 * t + q, at, :] = rows
                elif mode == "z":
                    ready[hops, core, along, at, :] = rows
                else:
                    ready[along, core, hops, at, :] = rows

            packed_tile(families, slice(t * LANES, (t + 1) * LANES), put)
            if group == 0:
                for q in range(4):
                    put(q, ROWS, router[...].astype(BF16))
        for copy in give(hops):
            copy.start()
    for hops in order:
        for copy in give(hops):
            copy.wait()


def packed(group, mode, me, args, *router):
    whole = pl.BlockSpec(memory_space=pl.ANY)
    if mode == "direct":
        rows = ROWS + 8 * len(router)
        shapes, ready = [(DESTS, rows, LANES)], (4, 8, rows, LANES)
    else:
        shapes, ready = [(2, 4, ROWS, LANES)] * 4, (4, 2, 4, ROWS, LANES)
    return pl.pallas_call(
        functools.partial(pack_kernel, group, mode),
        grid_spec=pltpu.PrefetchScalarGridSpec(
            num_scalar_prefetch=1,
            grid=(1,),
            in_specs=[whole] * 6 + [pl.BlockSpec((8, LANES), lambda i, me: (0, 0))] * len(router),
            out_specs=[whole] * len(shapes),
            scratch_shapes=[pltpu.VMEM((4, PACK, 64, 256), d) for d in (F32, BF16) * 3]
            + [pltpu.VMEM(ready, BF16)]
            + [pltpu.SemaphoreType.DMA((4, 6)), pltpu.SemaphoreType.DMA((4, 4))],
        ),
        out_shape=[pltpu.HBM(shape, BF16) for shape in shapes],
        compiler_params=pltpu.CompilerParams(vmem_limit_bytes=40 * 2**20),
    )(me, *args, *router)


def for_core_kernel(*refs):
    for k in range(4):
        refs[4][k] = refs[k][0]


def for_core(came):
    return pl.pallas_call(
        for_core_kernel,
        grid=(1,),
        in_specs=[pl.BlockSpec((1, 4, ROWS, LANES), lambda i: (1, 0, 0, 0))] * 4,
        out_specs=pl.BlockSpec((4, 4, ROWS, LANES), lambda i: (0, 0, 0, 0)),
        out_shape=jax.ShapeDtypeStruct((4, 4, ROWS, LANES), BF16),
        name="for_core",
    )(*came)


def for_second_kernel(*refs):
    came, other, outs = refs[:4], refs[4], refs[5:]
    for j in range(4):
        for k in range(4):
            outs[j][0, k] = came[k][0, j]
            outs[j][1, k] = other[k, j]


def for_second(came, other):
    return pl.pallas_call(
        for_second_kernel,
        grid=(1,),
        in_specs=[pl.BlockSpec((1, 4, ROWS, LANES), lambda i: (0, 0, 0, 0))] * 4
        + [pl.BlockSpec((4, 4, ROWS, LANES), lambda i: (0, 0, 0, 0))],
        out_specs=[pl.BlockSpec((2, 4, ROWS, LANES), lambda i: (0, 0, 0, 0))] * 4,
        out_shape=[jax.ShapeDtypeStruct((2, 4, ROWS, LANES), BF16)] * 4,
        name="for_second",
    )(*came, other)


def unpack_group(group, me, pieces, serves, scales, x):
    for kind in range(3):
        total = jnp.zeros((8, LANES), F32)
        for n, (_, load) in enumerate(pieces):
            for core in range(2):
                y = load(core, kind * 64, 64).astype(F32)
                factor = load(core, 192, 8).astype(F32)[kind : kind + 1]
                root = jnp.exp2(jnp.log2(jnp.abs(y)) * 0.0625) * factor
                v = jnp.where(y < 0, -root, root)
                x[n * LANES + core * 64 : n * LANES + (core + 1) * 64, :] = v
                total = total + jnp.sum((v * v).reshape(8, 8, LANES), axis=0)
        scale = jnp.sqrt(jnp.sum(total, axis=0, keepdims=True))
        inverse = 1.0 / scale
        place = [(b - me[3]) & 3 for b in range(4)]
        for b in range(4):
            scales[kind][pl.ds(group * PACK + place[b], 1), :] = scale[:, 32 * b : 32 * (b + 1)]
        for n, (tile, _) in enumerate(pieces):
            r = (x[n * LANES : (n + 1) * LANES, :] * inverse).T.astype(BF16)
            lanes = pl.ds(tile * LANES, LANES)
            if not isinstance(tile, int):
                lanes = pl.ds(pl.multiple_of(tile * LANES, LANES), LANES)
            for b in range(4):
                serves[kind][place[b], :, lanes] = r[32 * b : 32 * (b + 1)]


def carried(before, scales):
    for old, new in zip(before, scales):
        new[...] = old[...]


def direct_pieces(received):
    def load(n, core, first, rows):
        return received[2 * n + core, first : first + rows, :]

    return [(n, functools.partial(load, n)) for n in range(16)]


def unpack_first_kernel(group, me, received, *refs):
    router = refs[6]
    low = lax.broadcasted_iota(jnp.int32, (8, LANES), 1) < 64
    for n in range(16):
        a, b = (received[2 * n + core, ROWS : ROWS + 8, :].astype(F32) for core in range(2))
        a, b = jnp.where(low, a, pltpu.roll(b, 64, 1)), jnp.where(low, pltpu.roll(a, 64, 1), b)
        router[:, n * LANES : (n + 1) * LANES] = jnp.concatenate([a, b], axis=0).astype(BF16)
    unpack_group(group, me, direct_pieces(received), refs[:3], refs[3:6], refs[7])


def unpack_last_kernel(group, me, received, *refs):
    before, came, refs = refs[:3], refs[3:7], refs[10:]
    serves, scales, router, x = refs[:3], refs[3:6], refs[6], refs[7]
    for hop in range(4):
        router[(me[4] - hop) & 3] = came[hop][...]
    carried(before, scales)
    unpack_group(group, me, direct_pieces(received), serves, scales, x)


def unpack_relative_kernel(group, z_first, me, *refs):
    came, before, refs = refs[:4], refs[4:7], refs[10:]
    carried(before, refs[3:6])

    def load(second, first_hops, core, first, rows):
        return came[second][(core + me[2]) & 1, first_hops, pl.ds(first, rows), :]

    pieces = []
    for second in range(4):
        for first in range(4):
            z, y = (first, second) if z_first else (second, first)
            tile = ((me[0] - z) & 3) * 4 + ((me[1] - y) & 3)
            pieces.append((tile, functools.partial(load, second, first)))
    unpack_group(group, me, pieces, refs[:3], refs[3:6], refs[6])


def unpack_z_kernel(group, me, *refs):
    unpack_relative_kernel(group, True, me, *refs)


def unpack_y_kernel(group, me, *refs):
    unpack_relative_kernel(group, False, me, *refs)


def unpacking(kernel, group, me, blocked, serves, more_out=()):
    def full(x):
        return pl.BlockSpec(x.shape, lambda i, me: (0,) * len(x.shape))

    scale = jax.ShapeDtypeStruct((16, 32), F32)
    return pl.pallas_call(
        functools.partial(kernel, group),
        grid_spec=pltpu.PrefetchScalarGridSpec(
            num_scalar_prefetch=1,
            grid=(1,),
            in_specs=[full(b) for b in blocked] + [pl.BlockSpec(memory_space=pl.ANY)] * len(serves),
            out_specs=[pl.BlockSpec((PACK, 32, 2048), lambda i, me: (group, 0, 0))] * 3
            + [full(scale)] * 3
            + [full(o) for o in more_out],
            scratch_shapes=[pltpu.VMEM((2048, LANES), F32)],
        ),
        out_shape=[pltpu.HBM((16, 32, 2048), BF16)] * 3 + [scale] * 3 + list(more_out),
        input_output_aliases={1 + len(blocked) + n: n for n in range(len(serves))},
        compiler_params=pltpu.CompilerParams(vmem_limit_bytes=40 * 2**20),
    )(me, *blocked, *serves)


def moved(x, axis, hops):
    pairs = []
    for s in range(DESTS):
        z, y, core = s // 8, s // 2 % 4, s % 2
        if axis == "z":
            z = (z + hops) % 4
        elif axis == "y":
            y = (y + hops) % 4
        else:
            core = 1 - core
        pairs.append((s, 8 * z + 2 * y + core))
    return lax.ppermute(x, "rows", pairs)


def first_leg(x, axis):
    return [x[0]] + [moved(x[hops], axis, hops) for hops in range(1, 4)]


def over_cores(came):
    return moved(for_core(came), "core", 1)


def second_leg(came, other, axis):
    out = for_second(came, other)
    return [out[0]] + [moved(out[hops], axis, hops) for hops in range(1, 4)]


def shards(w_gate, avg_gate, w_up, avg_up, w_down, avg_down, router_weight, router_gain):
    args = (w_gate, avg_gate, w_up, avg_up, jnp.swapaxes(w_down, 1, 2), jnp.swapaxes(avg_down, 1, 2))
    args = [pltpu.with_memory_space_constraint(a, pltpu.HBM) for a in args]
    at, owner = lax.axis_index("rows"), lax.axis_index("owner")
    me = jnp.stack([at // 8, at // 2 % 4, at % 2, at % 4, owner]).astype(jnp.int32)
    part = (router_weight * router_gain[:, None]).astype(BF16).astype(F32).T
    part = jnp.concatenate([part[:8], part[8:]], axis=1)

    def exchanged(x):
        return lax.all_to_all(x, "rows", split_axis=0, concat_axis=0, tiled=True)

    z_send = packed(2, "z", me, args)
    z_came = first_leg(z_send, "z")
    y_send = packed(3, "y", me, args)
    y_came = first_leg(y_send, "y")
    payload = packed(0, "direct", me, args, part)[0]
    received_0 = exchanged(payload)
    payload = packed(1, "direct", me, args)[0]
    received_1 = exchanged(payload)
    z_other = over_cores(z_came)
    z_came = second_leg(z_came, z_other, "y")
    y_other = over_cores(y_came)
    y_came = second_leg(y_came, y_other, "z")

    half = [jax.ShapeDtypeStruct((16, 2048), BF16)]
    outs = unpacking(unpack_first_kernel, 0, me, [received_0], [], half)
    rows = outs[6]
    came = [rows] + [
        lax.ppermute(rows, "owner", [(s, (s + hop) % 4) for s in range(4)])
        for hop in range(1, 4)
    ]
    blocked = [*z_came, *outs[3:6]]
    outs = unpacking(unpack_z_kernel, 2, me, blocked, outs[:3])
    blocked = [*y_came, *outs[3:6]]
    outs = unpacking(unpack_y_kernel, 3, me, blocked, outs[:3])
    blocked = [received_1, *outs[3:6], *came]
    whole = [jax.ShapeDtypeStruct((4, 16, 2048), BF16)]
    *outs, router = unpacking(unpack_last_kernel, 1, me, blocked, outs[:3], whole)
    serve_router = router.reshape(64, 2048).T
    return (outs[0].swapaxes(1, 2), outs[1].swapaxes(1, 2), *outs[2:], serve_router)


def solution(mesh):
    return jax.shard_map(
        shards,
        mesh=mesh,
        in_specs=(
            P("owner", "rows", None),
            P("owner", "rows", None),
            P("owner", "rows", None),
            P("owner", "rows", None),
            P("owner", None, "rows"),
            P("owner", None, "rows"),
            P("rows", "owner"),
            P("rows"),
        ),
        out_specs=(
            P("owner", None, "rows"),
            P("owner", None, "rows"),
            P("owner", "rows", None),
            P("owner", "rows"),
            P("owner", "rows"),
            P("owner", "rows"),
            P(),
        ),
        check_vma=False,
    )
```
